128 devices in a mesh: node: 32 (over x, z, core), feat: 4 (over y).
Axes of the slice: x: 4, y: 4, z: 4, core: 2. Of those that a mesh axis runs over, the one named last changes fastest.
Arguments:
- features: bfloat16 [100, 32768], P('feat', 'node'), may hold values from -6 to 6
- edges_one: int32 [1024, 32768], P(None, 'node'), may hold values from 0 to 1, as said below
- w1_self: bfloat16 [100, 256], P('feat'), may hold values from -0.625 to 0.625
- w1_nbr: bfloat16 [100, 256], P('feat'), may hold values from -1.25 to 1.25
- need_blocks: int32 [32, 4], P('node'), may hold values from 0 to 31, as said below
- live_slots: int32 [32, 4], P('node'), may hold values from 0 to 1, as said below
- edges_two: int32 [4096, 32768], P(None, 'node'), may hold values from 0 to 1, as said below
- w2_self: bfloat16 [256, 47], P('feat'), may hold values from -0.375 to 0.375
- w2_nbr: bfloat16 [256, 47], P('feat'), may hold values from -0.5 to 0.5
- labels: int32 [32768], P('node'), may hold values from 0 to 46
Outputs:
- node_loss: float32 [32768], P('node')
- mean_loss: float32 [], replicated
The draws below stay inside these ranges and needn't reach their ends.
Inputs may be any that keep to these rules, and one draw needn't show every extreme that they name: `need_blocks`: row b holds 4 different blocks; its first entry is b, its second is b plus half the number of blocks, its third is b minus 1, and its entry k is b plus an offset that depends on k alone, modulo the number of blocks. `live_slots`: the first three entries of each row are 1. `edges_one`: each column has exactly 25 ones. `edges_two`: each column t has exactly 10 ones, all in rows of slots that live_slots marks as used for t's block.
All inputs are finite; a program needn't handle non-finite values.
Results may differ from the reference program's by a relative error of at most 0.00065.
Values may be sent and summed in bfloat16 or wider, within the bound.
A program may use at most 128 MiB of HBM per device.

```python
import jax
import jax.numpy as jnp
from jax import lax

F = 100
H = 256
C = 47
FAN1 = 25
FAN2 = 10
NEED = 4
BLK = 1024
NODES = 32768


def routing_tables(key):
    blocks = NODES // BLK
    offsets = jnp.arange(blocks, dtype=jnp.int32)
    scores = jax.random.randint(jax.random.fold_in(key, 12), (blocks,), 0, 2 ** 20) * blocks + offsets
    scores = jnp.where(offsets == blocks - 1, 2 ** 30 - 2, scores)
    scores = jnp.where(offsets == blocks // 2, 2 ** 30 - 1, scores)
    scores = jnp.where(offsets == 0, 2 ** 30, scores)
    chosen = lax.top_k(scores, NEED)[1].astype(jnp.int32)
    need = (jnp.arange(blocks, dtype=jnp.int32)[:, None] + chosen[None, :]) % blocks
    level = jax.random.randint(jax.random.fold_in(key, 13), (blocks, 1), 0, NEED + 1)
    coins = jax.random.randint(jax.random.fold_in(key, 14), (blocks, NEED), 0, NEED)
    slots = jnp.arange(NEED, dtype=jnp.int32)[None, :]
    live = jnp.where((slots < 3) | (coins < level), 1, 0).astype(jnp.int32)
    return (need.astype(jnp.int32), live)


def draw_need_blocks(key, part):
    return routing_tables(key)[0]


def draw_live_slots(key, part):
    return routing_tables(key)[1]


def draw_edges_two(key, part):
    need, live = routing_tables(key)
    width = NEED * BLK
    rows = jnp.arange(width, dtype=jnp.int32)[None, :]
    targets = jnp.arange(NODES, dtype=jnp.int32)
    used = live[targets // BLK][:, rows[0] // BLK]
    scores = jax.random.randint(jax.random.fold_in(key, 15), (NODES, width), 0, 2 ** 18) * width + rows
    scores = jnp.where(used == 1, scores, scores - 2 ** 30)
    chosen = lax.top_k(scores, FAN2)[1].astype(jnp.int32)
    return jnp.zeros((width, NODES), jnp.int32).at[chosen, targets[:, None]].set(1)


def draw_edges_one(key, part):
    rows = jnp.arange(BLK, dtype=jnp.int32)[None, :]
    targets = jnp.arange(NODES, dtype=jnp.int32)
    scores = jax.random.randint(jax.random.fold_in(key, 21), (NODES, BLK), 0, 2 ** 18) * BLK + rows
    chosen = lax.top_k(scores, FAN1)[1].astype(jnp.int32)
    return jnp.zeros((BLK, NODES), jnp.int32).at[chosen, targets[:, None]].set(1)


def place_ends(values, rng, least, top_value):
    spot = [jax.random.randint(jax.random.fold_in(rng, axis), (), 0, length) for axis, length in enumerate(values.shape)]
    longest = values.shape.index(max(values.shape))
    next_to = spot[:longest] + [(spot[longest] + 1) % values.shape[longest]] + spot[longest + 1:]
    return values.at[tuple(spot)].set(least).at[tuple(next_to)].set(top_value)


def levels(own_key, extent, shards, least, high):
    def one(axis_at, shards_of):
        heights = jax.random.uniform(jax.random.fold_in(jax.random.fold_in(own_key, 6), axis_at), (shards_of,), jnp.float32, least / len(shards), high / len(shards))
        return jnp.repeat(jnp.exp(heights), extent[axis_at] // shards_of).reshape((-1,) + (1,) * (len(extent) - axis_at - 1))

    level = one(*shards[0])
    for cut in shards[1:]:
        level = level * one(*cut)
    return level


def normal_values(stream_key, dims, deviation, most, split=(), kind=jnp.bfloat16):
    level = levels(stream_key, dims, split, -0.22, 0.18) if split else 1.0
    values = jax.random.normal(stream_key, dims, jnp.float32) * deviation * level
    return jnp.minimum(jnp.maximum(values, -most), most).astype(kind)


def setup_inputs(seed: int = 0) -> dict:
    keys = jax.random.split(jax.random.key(seed), 11)
    features = normal_values(keys[0], (F, NODES), 1.0, 6.0, ((0, 4), (1, 32)))
    edges_one = draw_edges_one(jax.random.fold_in(keys[10], 71), 0)
    w1_self = normal_values(keys[2], (F, H), F ** -0.5, 0.625, ((0, 4),))
    w1_nbr = normal_values(keys[3], (F, H), (F // 4) ** -0.5, 1.25, ((0, 4),))
    need_blocks = draw_need_blocks(jax.random.fold_in(keys[10], 71), 0)
    live_slots = draw_live_slots(jax.random.fold_in(keys[10], 71), 0)
    edges_two = draw_edges_two(jax.random.fold_in(keys[10], 71), 0)
    w2_self = normal_values(keys[7], (H, C), H ** -0.5, 0.375, ((0, 4),))
    w2_nbr = normal_values(keys[8], (H, C), (H // 2) ** -0.5, 0.5, ((0, 4),))
    labels = place_ends(jax.random.randint(keys[9], (NODES,), 0, C), jax.random.fold_in(keys[9], 1), 0, C - 1).astype(jnp.int32)
    return {"features": features, "edges_one": edges_one, "w1_self": w1_self, "w1_nbr": w1_nbr, "need_blocks": need_blocks, "live_slots": live_slots, "edges_two": edges_two, "w2_self": w2_self, "w2_nbr": w2_nbr, "labels": labels}


def reference(features, edges_one, w1_self, w1_nbr, need_blocks, live_slots, edges_two, w2_self, w2_nbr, labels):
    blocks = NODES // BLK
    inputs = features.reshape(F, blocks, BLK).transpose(1, 0, 2)
    firsts = edges_one.reshape(BLK, blocks, BLK).transpose(1, 0, 2)

    def first_layer(pair):
        block_x, adjacency = pair
        neighbour = (jnp.dot(block_x, adjacency.astype(jnp.bfloat16), preferred_element_type=jnp.float32) / FAN1).astype(jnp.bfloat16)
        before = jnp.dot(w1_self.T, block_x, preferred_element_type=jnp.float32)
        before = before + jnp.dot(w1_nbr.T, neighbour, preferred_element_type=jnp.float32)
        return jax.nn.relu(before).astype(jnp.bfloat16)

    hidden = lax.map(first_layer, (inputs, firsts))

    def second_layer(block):
        columns = lax.dynamic_slice_in_dim(edges_two, block * BLK, BLK, 1).reshape(NEED, BLK, BLK).astype(jnp.float32)
        weights = live_slots[block].astype(jnp.float32)
        sources = hidden[need_blocks[block]].astype(jnp.float32) * weights[:, None, None]
        gathered = jnp.einsum("khs,kst->ht", sources, columns, precision=lax.Precision.HIGHEST)
        logits = jnp.dot(w2_self.T, hidden[block], preferred_element_type=jnp.float32)
        logits = logits + jnp.dot(w2_nbr.T.astype(jnp.float32), gathered, precision=lax.Precision.HIGHEST) / FAN2
        block_labels = lax.dynamic_slice_in_dim(labels, block * BLK, BLK)
        class_ids = jnp.arange(C, dtype=jnp.int32)[:, None]
        picked = jnp.sum(jnp.where(class_ids == block_labels[None, :], logits, 0.0), 0)
        return jnp.log(jnp.sum(jnp.exp(logits), 0)) - picked

    node_loss = lax.map(second_layer, jnp.arange(blocks, dtype=jnp.int32)).reshape(NODES)
    mean_loss = jnp.sum(node_loss) / NODES
    return node_loss, mean_loss
```

```python
import functools

import jax
import jax.numpy as jnp
from jax import lax
from jax.experimental import pallas as pl
from jax.experimental.pallas import tpu as pltpu
from jax.sharding import PartitionSpec as P

FAN1 = 25
FAN2 = 10
MESH = pl.DeviceIdType.MESH
BF = jnp.bfloat16
F32 = jnp.float32
NODES = 32
FEAT = 4
ZN = 4
XN = 4


def kernel(
    feat_hbm, e1_hbm, w1s_hbm, w1n_hbm, need_hbm, live_hbm, e2_hbm, w2s_hbm, w2n_hbm, lab_hbm,
    loss_out, mean_out,
    feat_v, w1s_v, w1n_v, w2s_v, w2n_v, lab_v, need_s, live_s,
    e1_v, e2_v, e2_b, a_send, a_recv, w_buf, v_buf, wt, vt,
    sb, pc, zb, xb, lb, rb,
    in_sem, e1_sem, e2_sem, send_sem, a_sem, w_sem, v_sem, s_sem, pc_sem, z_sem, x_sem, l_sem, r_sem,
):
    n = lax.axis_index("node")
    f = lax.axis_index("feat")
    core = n % 2
    z = (n // 2) % ZN
    x = n // (2 * ZN)
    sends = []

    def send(src, dst, rsem, node, feat):
        copy = pltpu.make_async_remote_copy(
            src_ref=src, dst_ref=dst, send_sem=send_sem.at[len(sends)], recv_sem=rsem,
            device_id=(node, feat), device_id_type=MESH,
        )
        copy.start()
        sends.append(copy)

    def arrived(dst, rsem):
        pltpu.make_async_remote_copy(
            src_ref=dst, dst_ref=dst, send_sem=send_sem.at[0], recv_sem=rsem,
            device_id=(n, f), device_id_type=MESH,
        ).wait_recv()

    small = []
    for i, (src, dst) in enumerate([
        (feat_hbm, feat_v), (w1s_hbm, w1s_v), (w1n_hbm, w1n_v), (w2s_hbm, w2s_v), (w2n_hbm, w2n_v),
        (lab_hbm, lab_v), (need_hbm, need_s), (live_hbm, live_s),
    ]):
        c = pltpu.make_async_copy(src, dst, in_sem.at[i])
        c.start()
        small.append(c)
    e1c = []
    for i in range(4):
        c = pltpu.make_async_copy(e1_hbm.at[pl.ds(256 * i, 256), :], e1_v.at[pl.ds(256 * i, 256), :], e1_sem.at[i])
        c.start()
        e1c.append(c)
    e2c = []
    col = pl.multiple_of(f * 256, 256)
    for i in range(4):
        c = pltpu.make_async_copy(
            e2_hbm.at[pl.ds(1024 * i, 1024), pl.ds(col, 256)], e2_v.at[pl.ds(1024 * i, 1024), :], e2_sem.at[i])
        c.start()
        e2c.append(c)

    barrier = pltpu.get_barrier_semaphore()
    for d in range(1, NODES):
        pl.semaphore_signal(barrier, inc=1, device_id=((n + d) % NODES, f), device_id_type=MESH)
    for d in range(1, FEAT):
        pl.semaphore_signal(barrier, inc=1, device_id=(n, (f + d) % FEAT), device_id_type=MESH)

    for c in small:
        c.wait()
    w_buf[f, :, :] = jnp.zeros((64, 256), BF)
    w_buf[f, 0:25, :] = w1s_v[...]
    w_buf[f, 32:57, :] = w1n_v[...]
    v_buf[f, :, :] = jnp.zeros((64, 128), BF)
    v_buf[f, :, 0:47] = w2s_v[...]
    v_buf[f, :, 64:111] = w2n_v[...]
    a_send[...] = jnp.zeros((4, 64, 256), BF)
    acc = jnp.zeros((25, 1024), F32)
    feats = feat_v[...]
    for q in range(4):
        a_send[q, 0:25, :] = feats[:, 256 * q:256 * (q + 1)]
    for i in range(4):
        e1c[i].wait()
        rows = e1_v[256 * i:256 * (i + 1), :].astype(F32).astype(BF)
        acc = acc + jnp.dot(feats[:, 256 * i:256 * (i + 1)], rows, preferred_element_type=F32)
    agg = (acc / FAN1).astype(BF)
    for q in range(4):
        a_send[q, 32:57, :] = agg[:, 256 * q:256 * (q + 1)]

    pl.semaphore_wait(barrier, NODES - 1 + FEAT - 1)
    peers = [(f + d) % FEAT for d in (1, 3, 2)]
    for p in peers:
        send(w_buf.at[f], w_buf.at[f], w_sem.at[f], n, p)
    for p in peers:
        send(a_send.at[p], a_recv.at[f], a_sem.at[f], n, p)
    for p in peers:
        send(v_buf.at[f], v_buf.at[f], v_sem.at[f], n, p)
    a_recv[f, :, :] = a_send[f, :, :]

    for i in range(4):
        e2c[i].wait()
        e2_b[1024 * i:1024 * (i + 1), :] = e2_v[1024 * i:1024 * (i + 1), :].astype(F32).astype(BF)

    for p in peers:
        arrived(w_buf.at[p], w_sem.at[p])
    wt[...] = w_buf[...].reshape(256, 256).T
    for p in peers:
        arrived(a_recv.at[p], a_sem.at[p])
    before = jnp.dot(wt[...], a_recv[...].reshape(256, 256), preferred_element_type=F32)
    hidden = jnp.maximum(before, 0.0).astype(BF)
    for p in peers:
        arrived(v_buf.at[p], v_sem.at[p])
    vt[...] = v_buf[...].reshape(256, 128).T
    both = jnp.dot(vt[...], hidden, preferred_element_type=F32)
    logits = both[0:48, :]
    mine = both[64:112, :].astype(BF)
    sb[0, f, :, :] = mine
    pc[core, :, :] = mine

    partner = n + 1 - 2 * core
    send(pc.at[core], pc.at[core], pc_sem.at[0], partner, f)
    send(sb.at[0, f], sb.at[1, f], s_sem.at[1, f], (n + 16) % NODES, f)
    send(sb.at[0, f], sb.at[2, f], s_sem.at[2, f], (n + 1) % NODES, f)
    for p in peers:
        send(sb.at[0, f], sb.at[0, f], s_sem.at[0, f], n, p)

    source = (need_s[0, 3] + NODES) % NODES
    arrived(pc.at[1 - core], pc_sem.at[0])
    zb[z, :, :] = pc[source % 2]
    zpeers = [(z + d) % ZN for d in (1, 3, 2)]
    for q in zpeers:
        send(zb.at[z], zb.at[z], z_sem.at[z], x * 8 + q * 2 + core, f)
    for k in (1, 2):
        arrived(sb.at[k, f], s_sem.at[k, f])
        for p in peers:
            send(sb.at[k, f], sb.at[k, f], s_sem.at[k, f], n, p)
    for q in zpeers:
        arrived(zb.at[q], z_sem.at[q])
    xb[x, :, :] = zb[(source // 2) % ZN]
    xpeers = [(x + d) % XN for d in (1, 3, 2)]
    for q in xpeers:
        send(xb.at[x], xb.at[x], x_sem.at[x], q * 8 + z * 2 + core, f)
    gathered = jnp.zeros((48, 256), F32)

    def slot_term(k):
        term = jnp.zeros((48, 256), F32)
        for p in range(FEAT):
            r = 1024 * k + 256 * p
            term = term + jnp.dot(sb[k, p], e2_b[r:r + 256, :], preferred_element_type=F32)
        return term * live_s[0, k].astype(F32)

    for k in (0, 1, 2):
        for p in peers:
            arrived(sb.at[k, p], s_sem.at[k, p])
        gathered = gathered + slot_term(k)
    for q in xpeers:
        arrived(xb.at[q], x_sem.at[q])
    sb[3, f, :, :] = xb[source // (2 * ZN)]
    for p in peers:
        send(sb.at[3, f], sb.at[3, f], s_sem.at[3, f], n, p)
    for p in peers:
        arrived(sb.at[3, p], s_sem.at[3, p])
    gathered = gathered + slot_term(3)
    logits = logits + gathered / FAN2
    ids = lax.broadcasted_iota(jnp.int32, (48, 256), 0)
    lab = lab_v[f]
    lab = jnp.concatenate([lab[0:1, :], lab[1:2, :]], axis=1)
    picked = jnp.sum(jnp.where(ids == lab, logits, 0.0), axis=0, keepdims=True)
    total = jnp.sum(jnp.where(ids < 47, jnp.exp(logits), 0.0), axis=0, keepdims=True)
    loss = jnp.log(total) - picked
    lb[f, 0:1, :] = loss[:, 0:128]
    lb[f, 1:2, :] = loss[:, 128:256]
    for p in peers:
        send(lb.at[f], lb.at[f], l_sem.at[f], n, p)
    for p in peers:
        arrived(lb.at[p], l_sem.at[p])
    losses = lb[...]
    rb[n, :, :] = jnp.sum(jnp.sum(losses, axis=0), axis=0, keepdims=True)
    for d in range(1, NODES):
        q = (n + d) % NODES
        send(rb.at[n], rb.at[n], r_sem.at[n], q, f)
    out_copy = pltpu.make_async_copy(lb, loss_out, in_sem.at[0])
    out_copy.start()
    for d in range(1, NODES):
        q = (n + d) % NODES
        arrived(rb.at[q], r_sem.at[q])
    summed = jnp.sum(rb[...], axis=0)
    mean_out[...] = jnp.sum(summed, axis=1, keepdims=True) / (1024 * NODES)
    out_copy.wait()
    for copy in sends:
        copy.wait_send()


def local(features, edges_one, w1_self, w1_nbr, need_blocks, live_slots, edges_two, w2_self, w2_nbr, labels):
    any_spec = pl.BlockSpec(memory_space=pl.ANY)
    dma = pltpu.SemaphoreType.DMA
    loss, mean = pl.pallas_call(
        kernel,
        out_shape=(jax.ShapeDtypeStruct((4, 2, 128), F32), jax.ShapeDtypeStruct((1, 1), F32)),
        in_specs=[any_spec] * 10,
        out_specs=(any_spec, pl.BlockSpec(memory_space=pltpu.VMEM)),
        scratch_shapes=[
            pltpu.VMEM((25, 1024), BF), pltpu.VMEM((25, 256), BF), pltpu.VMEM((25, 256), BF),
            pltpu.VMEM((64, 47), BF), pltpu.VMEM((64, 47), BF), pltpu.VMEM((4, 2, 128), jnp.int32),
            pltpu.SMEM((1, 4), jnp.int32), pltpu.SMEM((1, 4), jnp.int32),
            pltpu.VMEM((1024, 1024), jnp.int32), pltpu.VMEM((4096, 256), jnp.int32), pltpu.VMEM((4096, 256), BF),
            pltpu.VMEM((4, 64, 256), BF), pltpu.VMEM((4, 64, 256), BF), pltpu.VMEM((4, 64, 256), BF),
            pltpu.VMEM((4, 64, 128), BF), pltpu.VMEM((256, 256), BF), pltpu.VMEM((128, 256), BF),
            pltpu.VMEM((4, 4, 48, 256), BF), pltpu.VMEM((2, 48, 256), BF), pltpu.VMEM((4, 48, 256), BF),
            pltpu.VMEM((4, 48, 256), BF), pltpu.VMEM((4, 2, 128), F32), pltpu.VMEM((NODES, 1, 128), F32),
            dma((8,)), dma((4,)), dma((4,)), dma((80,)), dma((4,)), dma((4,)), dma((4,)), dma((4, 4)),
            dma((1,)), dma((4,)), dma((4,)), dma((4,)), dma((NODES,)),
        ],
        compiler_params=pltpu.CompilerParams(collective_id=0, has_side_effects=True),
    )(features, edges_one, w1_self, w1_nbr, need_blocks, live_slots, edges_two, w2_self, w2_nbr,
      labels.reshape(4, 2, 128))
    return loss.reshape(1024), mean.reshape(())


def solution(mesh):
    return jax.shard_map(
        local,
        mesh=mesh,
        in_specs=(
            P("feat", "node"), P(None, "node"), P("feat", None), P("feat", None), P("node", None),
            P("node", None), P(None, "node"), P("feat", None), P("feat", None), P("node"),
        ),
        out_specs=(P("node"), P()),
        check_vma=False,
    )
```

```python
import math

import jax
import jax.numpy as jnp
from jax import lax
from jax.experimental import pallas as pl
from jax.experimental.pallas import tpu as pltpu
from jax.sharding import PartitionSpec as P

FAN1 = 25
FAN2 = 10
MESH = pl.DeviceIdType.MESH
BF = jnp.bfloat16
F32 = jnp.float32
NODES = 32
FEAT = 4
ZN = 4
XN = 4


def kernel(
    feat_hbm, e1_hbm, w1s_hbm, w1n_hbm, need_hbm, live_hbm, e2_hbm, w2s_hbm, w2n_hbm, lab_hbm,
    loss_out, part_out,
    feat_v, w1s_v, w1n_v, w2s_v, w2n_v, lab_v, need_s, live_s,
    e1_v, e2_v, e2_b, a_send, a_recv, w_buf, v_buf, wt, vt,
    sb, lg, z1, x1, x2, z2, gath, lb, pb, rb,
    in_sem, e1_sem, e2_sem, send_sem, a_sem, w_sem, v_sem, n_sem, y_sem, lg_sem, p_sem, r_sem,
):
    n = lax.axis_index("node")
    f = lax.axis_index("feat")
    core = n % 2
    z = (n // 2) % ZN
    x = n // (2 * ZN)
    other = 1 - core
    partner = n + 1 - 2 * core
    sent = []

    def node(xx, zz, cc):
        return xx * (2 * ZN) + zz * 2 + cc

    def send(src, dst, rsem, to, feat, ssem=0):
        pltpu.make_async_remote_copy(
            src_ref=src, dst_ref=dst, send_sem=send_sem.at[ssem], recv_sem=rsem,
            device_id=(to, feat), device_id_type=MESH,
        ).start()
        if ssem == 0:
            sent.append(math.prod(src.shape) * src.dtype.itemsize)

    def arrived(dst, rsem):
        pltpu.make_async_remote_copy(
            src_ref=dst, dst_ref=dst, send_sem=send_sem.at[0], recv_sem=rsem,
            device_id=(n, f), device_id_type=MESH,
        ).wait_recv()

    peers = [(f + d) % FEAT for d in (2, 1, 3)]
    zpeers = [(z + d) % ZN for d in (2, 1, 3)]
    xpeers = [(x + d) % XN for d in (2, 1, 3)]
    three = pl.ds(0, 3)

    small = []
    for i, (src, dst) in enumerate([
        (w1s_hbm, w1s_v), (w1n_hbm, w1n_v), (w2s_hbm, w2s_v), (w2n_hbm, w2n_v), (feat_hbm, feat_v),
        (need_hbm, need_s), (live_hbm, live_s), (lab_hbm, lab_v),
    ]):
        c = pltpu.make_async_copy(src, dst, in_sem.at[i])
        c.start()
        small.append(c)
    barrier = pltpu.get_barrier_semaphore()

    def hello(to, feat):
        pl.semaphore_signal(barrier, inc=1, device_id=(to, feat), device_id_type=MESH)

    for p in peers:
        hello(n, p)
    for q in zpeers:
        hello(node(x, q, core), f)
        hello(node(x, q, other), f)
    for q in xpeers:
        hello(node(q, z, core), f)
        hello(node(q, z, other), f)
    hello(partner, f)
    hello((n + 1) % NODES, f)
    hello((n + NODES - 1) % NODES, f)
    e1c = []
    for i in range(4):
        c = pltpu.make_async_copy(e1_hbm.at[pl.ds(256 * i, 256), :], e1_v.at[pl.ds(256 * i, 256), :], e1_sem.at[i])
        c.start()
        e1c.append(c)
    for c in small:
        c.wait()
    for h in range(2):
        cols = slice(128 * h, 128 * (h + 1))
        w_buf[f, h, :, :] = jnp.zeros((64, 128), BF)
        w_buf[f, h, 0:25, :] = w1s_v[:, cols]
        w_buf[f, h, 32:57, :] = w1n_v[:, cols]
    v_buf[f, 0, :, 0:64] = w2s_v[0:24, :]
    v_buf[f, 0, :, 64:128] = w2n_v[0:24, :]
    v_buf[f, 1, 23:24, :] = jnp.zeros((1, 128), BF)
    v_buf[f, 1, 0:23, 0:64] = w2s_v[24:47, :]
    v_buf[f, 1, 0:23, 64:128] = w2n_v[24:47, :]
    a_send[...] = jnp.zeros((4, 64, 256), BF)
    feats = feat_v[...]
    for q in range(4):
        a_send[q, 0:25, :] = feats[:, 256 * q:256 * (q + 1)]
    pl.semaphore_wait(barrier, 18)
    for p in peers:
        send(w_buf.at[f, core], w_buf.at[f, core], w_sem.at[core], n, p)
    for p in peers:
        send(v_buf.at[f, core], v_buf.at[f, core], v_sem.at[core], n, p)
    for p in peers:
        send(a_send.at[p, pl.ds(0, 32)], a_recv.at[f, pl.ds(0, 32)], a_sem.at[0], n, p)
    acc = jnp.zeros((25, 1024), F32)
    for i in range(4):
        e1c[i].wait()
        rows = e1_v[256 * i:256 * (i + 1), :].astype(F32).astype(BF)
        acc = acc + jnp.dot(feats[:, 256 * i:256 * (i + 1)], rows, preferred_element_type=F32)
    agg = (acc / FAN1).astype(BF)
    for q in range(4):
        a_send[q, 32:57, :] = agg[:, 256 * q:256 * (q + 1)]
    for p in peers:
        send(a_send.at[p, pl.ds(32, 32)], a_recv.at[f, pl.ds(32, 32)], a_sem.at[1], n, p)
    a_recv[f, :, :] = a_send[f, :, :]
    e2c = []
    for i in range(4):
        c = pltpu.make_async_copy(
            e2_hbm.at[pl.ds(1024 * i, 1024), :], e2_v.at[pl.ds(1024 * i, 1024), :], e2_sem.at[i])
        c.start()
        e2c.append(c)
    arrived(w_buf.at[three, 0], w_sem.at[core])
    for p in peers:
        send(w_buf.at[p, core], w_buf.at[p, core], w_sem.at[core], partner, f)
    arrived(v_buf.at[three, 0], v_sem.at[core])
    for p in peers:
        send(v_buf.at[p, core], v_buf.at[p, core], v_sem.at[core], partner, f)
    arrived(w_buf.at[three, 0], w_sem.at[other])
    for h in range(2):
        wt[128 * h:128 * (h + 1), :] = w_buf[:, h, :, :].reshape(256, 128).T
    arrived(v_buf.at[three, 0], v_sem.at[other])
    for p in range(FEAT):
        for h in range(2):
            vt[24 * h:24 * (h + 1), 64 * p:64 * (p + 1)] = v_buf[p, h, :, 0:64]
            vt[48 + 24 * h:72 + 24 * h, 64 * p:64 * (p + 1)] = v_buf[p, h, :, 64:128]
    arrived(a_recv.at[three, pl.ds(0, 32)], a_sem.at[0])
    arrived(a_recv.at[three, pl.ds(0, 32)], a_sem.at[1])
    before = jnp.dot(wt[...], a_recv[...].reshape(256, 256), preferred_element_type=F32)
    hidden = jnp.maximum(before, 0.0).astype(BF)
    both = jnp.dot(vt[...], hidden, preferred_element_type=F32)
    lg[f, :, :] = both[0:48, :]
    mine = both[48:96, :].astype(BF)
    for h in range(2):
        half = mine[:, 128 * h:128 * (h + 1)]
        sb[0, f, h, :, :] = half
    z1[z * 2 + core, :, :] = mine[:, 0:128]
    x1[x * 2 + core, :, :] = mine[:, 128:256]
    for q, r in zip(zpeers, xpeers):
        for c in (core, other):
            send(sb.at[0, f, 0], z1.at[z * 2 + core], p_sem.at[0], node(x, q, c), f)
            send(sb.at[0, f, 1], x1.at[x * 2 + core], p_sem.at[1], node(r, z, c), f)
    send(sb.at[0, f, 0], z1.at[z * 2 + core], p_sem.at[0], partner, f)
    send(sb.at[0, f, 1], x1.at[x * 2 + core], p_sem.at[1], partner, f)
    send(sb.at[0, f], sb.at[1, f], n_sem.at[0], (n + 16) % NODES, f)
    send(sb.at[0, f], sb.at[2, f], n_sem.at[1], (n + 1) % NODES, f)
    for p in peers:
        send(sb.at[0, f], sb.at[0, f], y_sem.at[0], n, p)
    for p in peers:
        send(lg.at[f], lg.at[f], lg_sem.at[0], n, p)

    source = (need_s[0, 3] + NODES) % NODES
    offset = (source - n + NODES) % NODES
    from_core = source % 2
    from_z = (source // 2) % ZN
    from_x = source // (2 * ZN)
    low = (z * 2 + from_core - offset + NODES) % (2 * ZN)
    via_x = ((x * (2 * ZN) + low + offset) // (2 * ZN)) % XN

    def convert(k):
        e2c[k].wait()

        def rows(i, carry):
            at = pl.ds(pl.multiple_of(1024 * k + 64 * i, 64), 64)
            e2_b[at, :] = e2_v[at, :].astype(F32).astype(BF)
            return carry

        lax.fori_loop(0, 16, rows, 0)

    for k in range(4):
        convert(k)
    seven = pl.ds(0, 7)
    arrived(z1.at[seven], p_sem.at[0])
    x2[x, :, :] = z1[from_z * 2 + from_core]
    for r in xpeers:
        send(x2.at[x], x2.at[x], p_sem.at[2], node(r, z, core), f)
    arrived(x1.at[seven], p_sem.at[1])
    z2[z, :, :] = x1[via_x * 2 + from_core]
    for r in zpeers:
        send(z2.at[z], z2.at[z], p_sem.at[3], node(x, r, core), f)
    for k in (1, 2):
        arrived(sb.at[k, f], n_sem.at[k - 1])
        for p in peers:
            send(sb.at[k, f], sb.at[k, f], y_sem.at[k], n, p)

    def slot_term(k):
        pieces = jnp.concatenate([sb[k, p, h] for p in range(FEAT) for h in range(2)], axis=1)
        term = jnp.dot(pieces, e2_b[1024 * k:1024 * (k + 1), :], preferred_element_type=F32)
        return term * (live_s[0, k].astype(F32) / FAN2)

    arrived(sb.at[0, three], y_sem.at[0])
    arrived(lg.at[three], lg_sem.at[0])
    own = jnp.concatenate([lg[p] for p in range(FEAT)], axis=1)
    gath[...] = own + slot_term(0)
    arrived(x2.at[three], p_sem.at[2])
    sb[3, f, 0, :, :] = x2[from_x]
    arrived(z2.at[three], p_sem.at[3])
    sb[3, f, 1, :, :] = z2[from_z]
    for p in peers:
        send(sb.at[3, f], sb.at[3, f], y_sem.at[3], n, p)
    for k in (1, 2):
        arrived(sb.at[k, three], y_sem.at[k])
        gath[...] = gath[...] + slot_term(k)
    arrived(sb.at[3, three], y_sem.at[3])
    logits = gath[...] + slot_term(3)
    ids = lax.broadcasted_iota(jnp.int32, (48, 1024), 0)
    lab = jnp.concatenate([lab_v[i // 2, i % 2:i % 2 + 1, :] for i in range(8)], axis=1)
    picked = jnp.sum(jnp.where(ids == lab, logits, 0.0), axis=0, keepdims=True)
    total = jnp.sum(jnp.where(ids < 47, jnp.exp(logits), 0.0), axis=0, keepdims=True)
    loss = jnp.log(total) - picked
    part = loss[:, 0:128]
    for i in range(1, 8):
        part = part + loss[:, 128 * i:128 * (i + 1)]
    rb[n, :, :] = part
    for d in [16] + [d for d in range(1, NODES) if d != 16]:
        send(rb.at[n], rb.at[n], r_sem.at[0], (n + d) % NODES, f, 1)
    for i in range(8):
        lb[i // 2, i % 2:i % 2 + 1, :] = loss[:, 128 * i:128 * (i + 1)]
    loss_copy = pltpu.make_async_copy(lb, loss_out, in_sem.at[0])
    loss_copy.start()
    tiles = sum(sent) // 4096
    assert tiles * 4096 == sum(sent)
    done = e2_v.at[pl.ds(0, 8 * tiles), pl.ds(0, 128)]
    pltpu.make_async_copy(done, done, send_sem.at[0]).wait()
    loss_copy.wait()
    most = rb.at[pl.ds(0, NODES - 1)]
    arrived(most, r_sem.at[0])
    pb[...] = jnp.sum(rb[...], axis=0)
    part_copy = pltpu.make_async_copy(pb, part_out, in_sem.at[1])
    part_copy.start()
    pltpu.make_async_copy(most, most, send_sem.at[1]).wait()
    part_copy.wait()


def finish(loss_ref, part_ref, loss_out, mean_out):
    loss_out[...] = loss_ref[...]
    mean_out[...] = jnp.sum(part_ref[...], axis=1, keepdims=True) / (1024 * NODES)


def local(features, edges_one, w1_self, w1_nbr, need_blocks, live_slots, edges_two, w2_self, w2_nbr, labels):
    any_spec = pl.BlockSpec(memory_space=pl.ANY)
    vmem_spec = pl.BlockSpec(memory_space=pltpu.VMEM)
    dma = pltpu.SemaphoreType.DMA
    vmem = pltpu.VMEM
    loss, part = pl.pallas_call(
        kernel,
        out_shape=(jax.ShapeDtypeStruct((4, 2, 128), F32), jax.ShapeDtypeStruct((1, 128), F32)),
        in_specs=[any_spec] * 10,
        out_specs=(any_spec, any_spec),
        scratch_shapes=[
            vmem((25, 1024), BF), vmem((25, 256), BF), vmem((25, 256), BF),
            vmem((47, 64), BF), vmem((47, 64), BF), vmem((4, 2, 128), jnp.int32),
            pltpu.SMEM((1, 4), jnp.int32), pltpu.SMEM((1, 4), jnp.int32),
            vmem((1024, 1024), jnp.int32), vmem((4096, 1024), jnp.int32), vmem((4096, 1024), BF),
            vmem((4, 64, 256), BF), vmem((4, 64, 256), BF), vmem((4, 2, 64, 128), BF),
            vmem((4, 2, 24, 128), BF), vmem((256, 256), BF), vmem((96, 256), BF),
            vmem((4, 4, 2, 48, 128), BF), vmem((4, 48, 256), F32), vmem((8, 48, 128), BF), vmem((8, 48, 128), BF),
            vmem((4, 48, 128), BF), vmem((4, 48, 128), BF), vmem((48, 1024), F32),
            vmem((4, 2, 128), F32), vmem((1, 128), F32), vmem((NODES, 1, 128), F32),
            dma((8,)), dma((4,)), dma((4,)), dma((2,)), dma((2,)), dma((2,)), dma((2,)), dma((2,)), dma((4,)),
            dma((1,)), dma((4,)), dma((1,)),
        ],
        compiler_params=pltpu.CompilerParams(collective_id=0, has_side_effects=True),
    )(features, edges_one, w1_self, w1_nbr, need_blocks, live_slots, edges_two, w2_self.T, w2_nbr.T,
      labels.reshape(4, 2, 128))
    loss, mean = pl.pallas_call(
        finish,
        out_shape=(jax.ShapeDtypeStruct((4, 2, 128), F32), jax.ShapeDtypeStruct((1, 1), F32)),
        in_specs=[vmem_spec, vmem_spec],
        out_specs=(vmem_spec, vmem_spec),
    )(loss, part)
    return loss.reshape(1024), mean.reshape(())


def solution(mesh):
    return jax.shard_map(
        local,
        mesh=mesh,
        in_specs=(
            P("feat", "node"), P(None, "node"), P("feat", None), P("feat", None), P("node", None),
            P("node", None), P(None, "node"), P("feat", None), P("feat", None), P("node"),
        ),
        out_specs=(P("node"), P()),
        check_vma=False,
    )
```
